128 devices in a mesh: seq: 32 (over x, y, core), tensor: 4 (over z).
Axes of the slice: x: 4, y: 4, z: 4, core: 2. Of those that a mesh axis runs over, the one named last changes fastest.
Arguments:
- tokens: bfloat16 [16384, 4096], P(('seq', 'tensor')), may hold values from -600 to 600
- gain: float32 [4096], replicated, may hold values from 0.5 to 1.5
- wq: bfloat16 [4096, 4096], P(None, 'tensor'), may hold values from -0.234375 to 0.234375
- wk: bfloat16 [4096, 1024], P(None, 'tensor'), may hold values from -0.09375 to 0.09375
- wv: bfloat16 [4096, 1024], P(None, 'tensor'), may hold values from -0.09375 to 0.09375
- wo: bfloat16 [4096, 4096], P('tensor'), may hold values from -0.25 to 0.25
- block_owner: int32 [128], replicated, may hold values from 0 to 32, as said below
Outputs:
- mixed: bfloat16 [16384, 4096], P(('seq', 'tensor'))
The draws below stay inside these ranges and needn't reach their ends.
Inputs may be any that keep to these rules, and one draw needn't show every extreme that they name: `block_owner`: block b holds tokens b * 128 to (b + 1) * 128 - 1. The first blocks, between 32 and 64 of them, have owner 0; from there the owner starts at 1 and rises by 0 or 1 from block to block, each value above 0 being one tool call; there are exactly 32 tool calls.
All inputs are finite; a program needn't handle non-finite values.
Results may differ from the reference program's by a relative error of at most 0.017.
Values may be sent and summed in bfloat16 or wider, within the bound.
A program may use at most 192 MiB of HBM per device.

```python
import math
import jax
import jax.numpy as jnp
from jax import lax

D = 4096
QH = 32
KV = 8
HD = 128
BLK = 128
TOK_DEV = 512
TOKENS = 16384
NB = 128


def draw_pair(key):
    query_key = jax.random.fold_in(key, 11)
    other_key = jax.random.fold_in(key, 12)
    query_w = jnp.clip(jax.random.normal(query_key, (D, QH * HD), jnp.float32), -6.0, 6.0)
    key_w = jnp.clip(jax.random.normal(other_key, (D, KV * HD), jnp.float32), -6.0, 6.0)
    query_w = (query_w * (2.5 / math.sqrt(D))).astype(jnp.bfloat16).astype(jnp.float32)
    key_w = (key_w * (1.0 / math.sqrt(D))).astype(jnp.bfloat16).astype(jnp.float32)
    return (query_w, key_w)


def draw_wq(key, part):
    return draw_pair(key)[0].astype(jnp.bfloat16)


def draw_wk(key, part):
    return draw_pair(key)[1].astype(jnp.bfloat16)


def draw_tokens(key, part):
    row_scale = jnp.exp(jax.random.uniform(jax.random.fold_in(key, 21), (TOKENS, 1), jnp.float32, 0.0, math.log(10.0)))
    col_scale = jnp.exp(jax.random.uniform(jax.random.fold_in(key, 22), (1, D), jnp.float32, 0.0, math.log(10.0)))
    base_key = jax.random.fold_in(key, 23)
    result = jnp.clip(jax.random.normal(base_key, (TOKENS, D), jnp.float32), -6.0, 6.0) * row_scale * col_scale
    return result.astype(jnp.bfloat16)


def draw_block_owner(key, part):
    size_key = jax.random.fold_in(key, 41)
    score_key = jax.random.fold_in(key, 42)
    context = jax.random.randint(size_key, (), NB // 4, NB // 2 + 1)
    block_ids = jnp.arange(NB, dtype=jnp.int32)
    candidate = block_ids > context
    raw_scores = jax.random.randint(score_key, (NB,), 0, NB)
    scores = jnp.where(candidate, raw_scores * NB + block_ids, NB * NB + block_ids).astype(jnp.int32)
    order = jnp.argsort(scores, stable=True)
    ranking = jnp.argsort(order, stable=True).astype(jnp.int32)
    chosen = (ranking < NB // 4 - 1).astype(jnp.int32)
    starts = jnp.where(block_ids == context, 1, jnp.where(candidate, chosen, 0))
    return jnp.cumsum(starts).astype(jnp.int32)


def level_of(stream_key, shape, split, smallest, high):
    def one(dim, blocks):
        draws = jax.random.uniform(jax.random.fold_in(jax.random.fold_in(stream_key, 6), dim), (blocks,), jnp.float32, smallest / len(split), high / len(split))
        return jnp.repeat(jnp.exp(draws), shape[dim] // blocks).reshape((-1,) + (1,) * (len(shape) - dim - 1))

    level = one(*split[0])
    for cut in split[1:]:
        level = level * one(*cut)
    return level


def normal_values(own_key, extent, deviation, most, split=(), held_as=jnp.bfloat16):
    values = deviation * jax.random.normal(own_key, extent, jnp.float32)
    if split:
        values = values * level_of(own_key, extent, split, -0.22, 0.18)
    return jnp.clip(values, -most, most).astype(held_as)


def setup_inputs(seed: int = 0) -> dict:
    splits = jax.random.split(jax.random.key(seed), 8)
    tokens = draw_tokens(jax.random.fold_in(splits[7], 71), 0)
    gain = jnp.clip(1.0 + 0.1 * jax.random.normal(splits[1], (D,), jnp.float32), 0.5, 1.5)
    wq = draw_wq(jax.random.fold_in(splits[7], 71), 0)
    wk = draw_wk(jax.random.fold_in(splits[7], 71), 0)
    wv = normal_values(splits[4], (D, KV * HD), D ** -0.5, 0.09375, ((1, 4),))
    wo = normal_values(splits[5], (QH * HD, D), (QH * HD // 8) ** -0.5, 0.25, ((0, 4),))
    block_owner = draw_block_owner(jax.random.fold_in(splits[7], 71), 0)
    return dict(tokens=tokens, gain=gain, wq=wq, wk=wk, wv=wv, wo=wo, block_owner=block_owner)


norm_eps = 1e-05
rope_base = 500000.0

def owner_of(position, owners):
    block_ids = jnp.arange(owners.shape[0], dtype=jnp.int32)
    matches = (position // BLK)[:, None] == block_ids[None, :]
    return lax.optimization_barrier(jnp.sum(jnp.where(matches, owners[None, :], 0), axis=1)).astype(jnp.int32)

def rope_position(position, owners):
    token_owner = owner_of(position, owners)
    context = BLK * jnp.sum((owners == 0).astype(jnp.int32))
    before = BLK * lax.optimization_barrier(jnp.sum((owners[None, :] < token_owner[:, None]).astype(jnp.int32), axis=1))
    return jnp.where(token_owner == 0, position, context + position - before).astype(jnp.int32)

def rotate(vectors, position):
    half_size = vectors.shape[-1] // 2
    exponent = jnp.arange(half_size, dtype=jnp.float32) * (2.0 / vectors.shape[-1])
    frequency = jnp.exp(-exponent * math.log(rope_base))
    angles = position.astype(jnp.float32)[:, None] * frequency[None, :]
    cosine = jnp.cos(angles)[:, None, :]
    sine_part = jnp.sin(angles)[:, None, :]
    first_half = vectors[..., :half_size]
    second = vectors[..., half_size:]
    return jnp.concatenate([first_half * cosine - second * sine_part, second * cosine + first_half * sine_part], axis=-1)

def reference(tokens, gain, wq, wk, wv, wo, block_owner):
    total_rows = tokens.shape[0]
    widened = tokens.astype(jnp.float32)
    normed = (widened * lax.rsqrt(lax.optimization_barrier(jnp.mean(widened * widened, axis=-1, keepdims=True)) + norm_eps) * gain).astype(jnp.bfloat16)
    position = jnp.arange(total_rows, dtype=jnp.int32)
    rotary = rope_position(position, block_owner)
    token_owner = owner_of(position, block_owner)
    queries = rotate(jnp.dot(normed, wq, preferred_element_type=jnp.float32).reshape(total_rows, QH, HD), rotary).astype(jnp.bfloat16)
    key_rows = rotate(jnp.dot(normed, wk, preferred_element_type=jnp.float32).reshape(total_rows, KV, HD), rotary).astype(jnp.bfloat16)
    value_rows = jnp.dot(normed, wv, preferred_element_type=jnp.float32).reshape(total_rows, KV, HD).astype(jnp.bfloat16)
    span = 4 * TOK_DEV
    blocks = total_rows // span
    group_size = QH // KV
    scale = 1.0 / math.sqrt(HD)
    query_blocks = queries.reshape(blocks, span, KV, group_size, HD)
    keys_by_head = key_rows.transpose(1, 0, 2)
    values_by_head = value_rows.transpose(1, 0, 2)

    def one_block(block_index):
        query_pos = block_index * span + jnp.arange(span, dtype=jnp.int32)
        query_owner = lax.dynamic_slice_in_dim(token_owner, block_index * span, span, 0)
        allowed = (position[None, :] <= query_pos[:, None]) & ((token_owner[None, :] == 0) | (token_owner[None, :] == query_owner[:, None]))
        block_rows = lax.dynamic_index_in_dim(query_blocks, block_index, 0, keepdims=False).transpose(1, 0, 2, 3)

        def one_head(operands):
            query_head, key_head, value_head = operands
            scores = jnp.einsum('qre,ne->qrn', query_head.astype(jnp.float32), key_head.astype(jnp.float32)) * scale
            visible = allowed[:, None, :]
            scores = jnp.where(visible, scores, -1e+30)
            highest = lax.optimization_barrier(jnp.max(scores, axis=-1, keepdims=True))
            weights = jnp.where(visible, jnp.exp(scores - highest), 0.0)
            denominator = lax.optimization_barrier(jnp.sum(weights, axis=-1))
            rounded_weights = lax.optimization_barrier(weights.astype(jnp.bfloat16)).astype(jnp.float32)
            summed = jnp.einsum('qrn,ne->qre', rounded_weights, value_head.astype(jnp.float32))
            return (summed / denominator[..., None]).astype(jnp.bfloat16)
        return lax.map(one_head, (block_rows, keys_by_head, values_by_head))
    outputs = lax.map(one_block, jnp.arange(blocks, dtype=jnp.int32))
    attended = outputs.transpose(0, 2, 1, 3, 4).reshape(total_rows, QH * HD)
    return jnp.dot(attended, wo, preferred_element_type=jnp.float32).astype(jnp.bfloat16)
```

```python
import functools
import math

import jax
import jax.numpy as jnp
from jax import lax
from jax.experimental import pallas as pl
from jax.experimental.layout import Layout, with_layout_constraint
from jax.experimental.pallas import tpu as pltpu
from jax.sharding import PartitionSpec as P

HD = 128
BLK = 128
LOWEST = -1e30


norm_eps = 1e-05
rope_base = 500000.0


def owner_of(position, owners):
    block_ids = jnp.arange(owners.shape[0], dtype=jnp.int32)
    matches = (position // BLK)[:, None] == block_ids[None, :]
    return jnp.sum(jnp.where(matches, owners[None, :], 0), axis=1)


def rope_position(position, owners):
    token_owner = owner_of(position, owners)
    context = BLK * jnp.sum((owners == 0).astype(jnp.int32))
    before = BLK * jnp.sum((owners[None, :] < token_owner[:, None]).astype(jnp.int32), axis=1)
    return jnp.where(token_owner == 0, position, context + position - before)


def rotate(vectors, position):
    half_size = vectors.shape[-1] // 2
    exponent = jnp.arange(half_size, dtype=jnp.float32) * (2.0 / vectors.shape[-1])
    frequency = jnp.exp(-exponent * math.log(rope_base))
    angles = position.astype(jnp.float32)[:, None] * frequency[None, :]
    cosine = jnp.cos(angles)[:, None, :]
    sine_part = jnp.sin(angles)[:, None, :]
    first_half = vectors[..., :half_size]
    second = vectors[..., half_size:]
    return jnp.concatenate(
        [first_half * cosine - second * sine_part, second * cosine + first_half * sine_part],
        axis=-1,
    )


def attend_kernel(plan_ref, q_hbm, kv_hbm, wo_hbm, o_ref, qbuf, kvbuf, wobuf, acc, total_s, max_s, kv_sems, q_sem, wo_sem, *, full_blocks, tail_blocks, rows_per_step):
    context, first_own, count, last, row = [plan_ref[i] for i in range(5)]
    heads = qbuf.shape[1] // HD
    groups = kvbuf.shape[3] // (2 * HD)
    per_group = heads // groups
    full_steps = (count - 1) // full_blocks
    rest = count - full_steps * full_blocks
    steps = full_steps + (rest + tail_blocks - 1) // tail_blocks
    wo_copy = pltpu.make_async_copy(wo_hbm, wobuf, wo_sem)
    q_copy = pltpu.make_async_copy(q_hbm.at[pl.ds(pl.multiple_of(row, BLK), BLK)], qbuf, q_sem)

    def start_of(step):
        return jnp.where(step < full_steps, step * full_blocks, full_steps * full_blocks + (step - full_steps) * tail_blocks)

    def fetch(step, slot):
        base = start_of(step)

        def one(j):
            at = base + j
            block = jnp.where(at < context, at, jnp.minimum(first_own + at - context, last))
            pltpu.make_async_copy(kv_hbm.at[block], kvbuf.at[slot, j], kv_sems.at[slot]).start()

        for j in range(tail_blocks):
            one(j)

        if full_blocks > tail_blocks:
            @pl.when(step < full_steps)
            def _():
                for j in range(tail_blocks, full_blocks):
                    one(j)

    q_copy.start()
    fetch(0, 0)
    wo_copy.start()
    acc[...] = jnp.zeros_like(acc)
    total_s[...] = jnp.zeros_like(total_s)
    max_s[...] = jnp.full_like(max_s, LOWEST)
    q_copy.wait()

    def absorb(step, blocks, masked):
        slot = lax.rem(step, 2)

        @pl.when(step + 1 < steps)
        def _():
            fetch(step + 1, 1 - slot)

        pltpu.make_async_copy(kv_hbm.at[pl.ds(0, blocks)], kvbuf.at[slot, pl.ds(0, blocks)], kv_sems.at[slot]).wait()
        keys = blocks * BLK
        if masked:
            column = lax.broadcasted_iota(jnp.int32, (BLK, keys), 1) + (start_of(step) - (count - 1)) * BLK
            visible = column <= lax.broadcasted_iota(jnp.int32, (BLK, keys), 0)
            visible = jnp.concatenate([visible] * rows_per_step, axis=0)
        for g in range(groups):
            k = kvbuf[slot, :blocks, :, g * HD:(g + 1) * HD].reshape(keys, HD)
            v = kvbuf[slot, :blocks, :, (groups + g) * HD:(groups + g + 1) * HD].reshape(keys, HD)
            v_one = jnp.concatenate([v, jnp.ones_like(v)], axis=1)
            for first in range(g * per_group, (g + 1) * per_group, rows_per_step):
                q = jnp.concatenate([qbuf[:, h * HD:(h + 1) * HD] for h in range(first, first + rows_per_step)], axis=0)
                s = lax.dot_general(q, k, (((1,), (1,)), ((), ())), preferred_element_type=jnp.float32)
                if masked:
                    s = jnp.where(visible, s, LOWEST)
                rows = pl.ds(first * BLK, rows_per_step * BLK)
                top = s[:, :BLK]
                for j in range(1, blocks):
                    top = jnp.maximum(top, s[:, j * BLK:(j + 1) * BLK])
                old = max_s[rows]
                new = jnp.maximum(old, jnp.max(top, axis=1, keepdims=True))
                factor = jnp.exp2(old - new)
                p = jnp.concatenate([jnp.exp2(s[:, j * BLK:(j + 1) * BLK] - new).astype(jnp.bfloat16) for j in range(blocks)], axis=1)
                r = jnp.dot(p, v_one, preferred_element_type=jnp.float32)
                acc[rows] = acc[rows] * factor + r[:, :HD]
                total_s[rows] = total_s[rows] * factor + r[:, HD:]
                max_s[rows] = new

    def full(step, carry):
        absorb(step, full_blocks, False)
        return carry

    def tail(step, carry):
        absorb(step, tail_blocks, True)
        return carry

    lax.fori_loop(0, full_steps, full, 0)
    lax.fori_loop(full_steps, steps, tail, 0)
    attended = jnp.concatenate(
        [(acc[pl.ds(h * BLK, BLK)] / total_s[pl.ds(h * BLK, BLK)]).astype(jnp.bfloat16) for h in range(heads)], axis=1)
    wo_copy.wait()
    o_ref[...] = jnp.dot(attended, wobuf[...], preferred_element_type=jnp.float32).astype(jnp.bfloat16)


def attend(plan, q, kv, wo, full_blocks=16, tail_blocks=4, rows_per_step=2):
    width = wo.shape[1]
    heads = q.shape[1] // HD
    any_space = pl.BlockSpec(memory_space=pl.ANY)
    state = pltpu.VMEM((heads * BLK, HD), jnp.float32)
    return pl.pallas_call(
        functools.partial(attend_kernel, full_blocks=full_blocks, tail_blocks=tail_blocks, rows_per_step=rows_per_step),
        out_shape=jax.ShapeDtypeStruct((BLK, width), jnp.bfloat16),
        in_specs=[pl.BlockSpec(memory_space=pltpu.SMEM), any_space, any_space, any_space],
        out_specs=pl.BlockSpec(memory_space=pltpu.VMEM),
        scratch_shapes=[
            pltpu.VMEM((BLK, heads * HD), jnp.bfloat16),
            pltpu.VMEM((2, full_blocks, BLK, kv.shape[2]), jnp.bfloat16),
            pltpu.VMEM(wo.shape, jnp.bfloat16),
            state, state, state,
            pltpu.SemaphoreType.DMA((2,)),
            pltpu.SemaphoreType.DMA,
            pltpu.SemaphoreType.DMA,
        ],
        compiler_params=pltpu.CompilerParams(vmem_limit_bytes=56 * 1024 * 1024),
        cost_estimate=pl.CostEstimate(flops=8 * heads * BLK * 6400 * HD, bytes_accessed=16 << 20, transcendentals=heads * BLK * 6400),
    )(plan, q, kv, wo)


def plan_of(block, row, owners):
    owner = jnp.sum(jnp.where(jnp.arange(owners.shape[0]) == block, owners, 0))
    shared = jnp.sum((owners == 0).astype(jnp.int32))
    first_own = jnp.sum((owners < owner).astype(jnp.int32))
    context = jnp.where(owner == 0, block + 1, shared)
    count = jnp.where(owner == 0, block + 1, shared + block - first_own + 1)
    return jnp.stack([context, first_own, count, block, row]).astype(jnp.int32)


def per_device(tokens, gain, wq, wk, wv, wo, block_owner):
    parts = lax.axis_size("tensor")
    seq_index = lax.axis_index("seq")
    part = lax.axis_index("tensor")
    local_rows = tokens.shape[0]
    tok_rows = local_rows * parts
    q_heads = wq.shape[1] // HD
    kv_heads = wk.shape[1] // HD
    widened = tokens.astype(jnp.float32)
    normed = (
        widened * lax.rsqrt(jnp.mean(widened * widened, axis=-1, keepdims=True) + norm_eps) * gain
    ).astype(jnp.bfloat16)
    rows = lax.all_gather(normed, "tensor", axis=0, tiled=True)
    position = seq_index * tok_rows + jnp.arange(tok_rows, dtype=jnp.int32)
    rotary = rope_position(position, block_owner)
    keys = rotate(
        jnp.dot(rows, wk, preferred_element_type=jnp.float32).reshape(tok_rows, kv_heads, HD), rotary
    ).astype(jnp.bfloat16)
    values = jnp.dot(rows, wv, preferred_element_type=jnp.float32).astype(jnp.bfloat16)
    own = jnp.concatenate([keys.reshape(tok_rows, kv_heads * HD), values], axis=1)
    own = with_layout_constraint(own, Layout(major_to_minor=(0, 1)))
    gathered = lax.all_gather(own, "seq", axis=0, tiled=True)
    queries = rotate(
        jnp.dot(rows, wq, preferred_element_type=jnp.float32).reshape(tok_rows, q_heads, HD), rotary
    )
    queries = (queries * (math.log2(math.e) / math.sqrt(HD))).astype(jnp.bfloat16)
    queries = queries.reshape(tok_rows, q_heads * HD)
    kv = gathered.reshape(-1, BLK, own.shape[1])
    total = None
    pieces = []
    for shift in (2, 1, 3, 0):
        group = lax.rem(part + shift, parts)
        plan = plan_of(seq_index * parts + group, group * BLK, block_owner)
        piece = attend(plan, queries, kv, wo)
        if shift:
            piece = lax.ppermute(piece, "tensor", [(i, (i + shift) % parts) for i in range(parts)])
        pieces.append(piece)
    total = sum(piece.astype(jnp.float32) for piece in pieces[::-1])
    return total.astype(jnp.bfloat16)


def solution(mesh):
    in_specs = (
        P(("seq", "tensor"), None),
        P(),
        P(None, "tensor"),
        P(None, "tensor"),
        P(None, "tensor"),
        P("tensor", None),
        P(),
    )
    out_specs = P(("seq", "tensor"), None)
    return jax.shard_map(
        per_device, mesh=mesh, in_specs=in_specs, out_specs=out_specs, check_vma=False
    )
```

```python
import functools
import math

import jax
import jax.numpy as jnp
from jax import lax
from jax.experimental import pallas as pl
from jax.experimental.layout import Layout, with_layout_constraint
from jax.experimental.pallas import tpu as pltpu
from jax.sharding import PartitionSpec as P

HD = 128
BLK = 128
LOWEST = -1e30


norm_eps = 1e-05
rope_base = 500000.0


def rotate(vectors, position):
    half_size = vectors.shape[-1] // 2
    exponent = jnp.arange(half_size, dtype=jnp.float32) * (2.0 / vectors.shape[-1])
    frequency = jnp.exp(-exponent * math.log(rope_base))
    angles = position.astype(jnp.float32)[:, None] * frequency[None, :]
    cosine = jnp.cos(angles)[:, None, :]
    sine_part = jnp.sin(angles)[:, None, :]
    first_half = vectors[..., :half_size]
    second = vectors[..., half_size:]
    return jnp.concatenate(
        [first_half * cosine - second * sine_part, second * cosine + first_half * sine_part],
        axis=-1,
    )


def attend_kernel(plan_ref, q_hbm, own_hbm, beside_hbm, across_hbm, wo_hbm, o_ref, qbuf, kvbuf, wobuf, acc, total_s, max_s, kv_sems, q_sem, wo_sem, *, full_blocks, tail_blocks, rows_per_step):
    context, first_own, count, last, part = [plan_ref[i] for i in range(5)]
    heads = qbuf.shape[1] // HD
    groups = kvbuf.shape[3] // (2 * HD)
    per_group = heads // groups
    full_steps = (count - 1) // full_blocks
    rest = count - full_steps * full_blocks
    steps = full_steps + (rest + tail_blocks - 1) // tail_blocks
    wo_copy = pltpu.make_async_copy(wo_hbm, wobuf, wo_sem)
    q_copy = pltpu.make_async_copy(q_hbm, qbuf, q_sem)

    def start_of(step):
        return jnp.where(step < full_steps, step * full_blocks, full_steps * full_blocks + (step - full_steps) * tail_blocks)

    def fetch(step, slot):
        base = start_of(step)

        def one(j):
            at = base + j
            block = jnp.where(at < context, at, jnp.minimum(first_own + at - context, last))
            shard = block // 4
            place = lax.rem(block - part + 4, 4)

            @pl.when(place == 0)
            def _():
                pltpu.make_async_copy(own_hbm.at[shard], kvbuf.at[slot, j], kv_sems.at[slot]).start()

            @pl.when(lax.rem(place, 2) == 1)
            def _():
                at_beside = 2 * shard + (place == 1).astype(jnp.int32)
                pltpu.make_async_copy(beside_hbm.at[at_beside], kvbuf.at[slot, j], kv_sems.at[slot]).start()

            @pl.when(place == 2)
            def _():
                pltpu.make_async_copy(across_hbm.at[shard], kvbuf.at[slot, j], kv_sems.at[slot]).start()

        def each(j, carry):
            one(j)
            return carry

        lax.fori_loop(0, jnp.where(step < full_steps, full_blocks, tail_blocks), each, 0)

    q_copy.start()
    fetch(0, 0)
    wo_copy.start()
    acc[...] = jnp.zeros_like(acc)
    total_s[...] = jnp.zeros_like(total_s)
    max_s[...] = jnp.full_like(max_s, LOWEST)
    q_copy.wait()

    def absorb(step, blocks, masked):
        slot = lax.rem(step, 2)

        @pl.when(step + 1 < steps)
        def _():
            fetch(step + 1, 1 - slot)

        pltpu.make_async_copy(own_hbm.at[pl.ds(0, blocks)], kvbuf.at[slot, pl.ds(0, blocks)], kv_sems.at[slot]).wait()
        keys = blocks * BLK
        if masked:
            column = lax.broadcasted_iota(jnp.int32, (BLK, keys), 1) + (start_of(step) - (count - 1)) * BLK
            visible = column <= lax.broadcasted_iota(jnp.int32, (BLK, keys), 0)
            visible = jnp.concatenate([visible] * rows_per_step, axis=0)
        for g in range(groups):
            k = kvbuf[slot, :blocks, :, g * HD:(g + 1) * HD].reshape(keys, HD)
            v = kvbuf[slot, :blocks, :, (groups + g) * HD:(groups + g + 1) * HD].reshape(keys, HD)
            v_one = jnp.concatenate([v, jnp.ones_like(v)], axis=1)
            for first in range(g * per_group, (g + 1) * per_group, rows_per_step):
                q = jnp.concatenate([qbuf[:, h * HD:(h + 1) * HD] for h in range(first, first + rows_per_step)], axis=0)
                s = lax.dot_general(q, k, (((1,), (1,)), ((), ())), preferred_element_type=jnp.float32)
                if masked:
                    s = jnp.where(visible, s, LOWEST)
                rows = pl.ds(first * BLK, rows_per_step * BLK)
                top = s[:, :BLK]
                for j in range(1, blocks):
                    top = jnp.maximum(top, s[:, j * BLK:(j + 1) * BLK])
                old = max_s[rows]
                new = jnp.maximum(old, jnp.max(top, axis=1, keepdims=True))
                factor = jnp.exp2(old - new)
                p = jnp.concatenate([jnp.exp2(s[:, j * BLK:(j + 1) * BLK] - new).astype(jnp.bfloat16) for j in range(blocks)], axis=1)
                r = jnp.dot(p, v_one, preferred_element_type=jnp.float32)
                acc[rows] = acc[rows] * factor + r[:, :HD]
                total_s[rows] = total_s[rows] * factor + r[:, HD:]
                max_s[rows] = new

    def full(step, carry):
        absorb(step, full_blocks, False)
        return carry

    def tail(step, carry):
        absorb(step, tail_blocks, True)
        return carry

    lax.fori_loop(0, full_steps, full, 0)
    lax.fori_loop(full_steps, steps, tail, 0)
    attended = jnp.concatenate(
        [(acc[pl.ds(h * BLK, BLK)] / total_s[pl.ds(h * BLK, BLK)]).astype(jnp.bfloat16) for h in range(heads)], axis=1)
    wo_copy.wait()
    o_ref[...] = jnp.dot(attended, wobuf[...], preferred_element_type=jnp.float32).astype(jnp.bfloat16)


def attend(plan, q, own, beside, across, wo, full_blocks=16, tail_blocks=4, rows_per_step=2):
    width = wo.shape[1]
    heads = q.shape[1] // HD
    any_space = pl.BlockSpec(memory_space=pl.ANY)
    state = pltpu.VMEM((heads * BLK, HD), jnp.float32)
    return pl.pallas_call(
        functools.partial(attend_kernel, full_blocks=full_blocks, tail_blocks=tail_blocks, rows_per_step=rows_per_step),
        out_shape=jax.ShapeDtypeStruct((BLK, width), jnp.bfloat16),
        in_specs=[pl.BlockSpec(memory_space=pltpu.SMEM), any_space, any_space, any_space, any_space, any_space],
        out_specs=pl.BlockSpec(memory_space=pltpu.VMEM),
        scratch_shapes=[
            pltpu.VMEM((BLK, heads * HD), jnp.bfloat16),
            pltpu.VMEM((2, full_blocks, BLK, own.shape[2]), jnp.bfloat16),
            pltpu.VMEM(wo.shape, jnp.bfloat16),
            state, state, state,
            pltpu.SemaphoreType.DMA((2,)),
            pltpu.SemaphoreType.DMA,
            pltpu.SemaphoreType.DMA,
        ],
        compiler_params=pltpu.CompilerParams(vmem_limit_bytes=56 * 1024 * 1024),
        cost_estimate=pl.CostEstimate(flops=2 * heads * BLK * 6400 * HD, bytes_accessed=4 << 20, transcendentals=0),
    )(plan, q, own, beside, across, wo)


def plan_of(blocks, part, owners):
    ids = jnp.arange(owners.shape[0], dtype=jnp.int32)
    owner = jnp.sum(jnp.where(ids[None, :] == blocks[:, None], owners[None, :], 0), axis=1)
    shared = jnp.sum((owners == 0).astype(jnp.int32))
    before = jnp.sum((owners[None, :] < owner[:, None]).astype(jnp.int32), axis=1)
    is_shared = owner == 0
    context = jnp.where(is_shared, blocks + 1, shared)
    count = jnp.where(is_shared, blocks + 1, shared + blocks - before + 1)
    plan = jnp.stack([context, before, count, blocks, jnp.full_like(blocks, part)]).astype(jnp.int32)
    first_position = BLK * jnp.where(is_shared, blocks, shared + blocks - before)
    return plan, first_position


def per_device(tokens, gain, wq, wk, wv, wo, block_owner):
    parts = lax.axis_size("tensor")
    seq_index = lax.axis_index("seq")
    part = lax.axis_index("tensor")
    q_heads = wq.shape[1] // HD
    kv_heads = wk.shape[1] // HD

    def moved(array, shift):
        return lax.ppermute(array, "tensor", [(i, (i + shift) % parts) for i in range(parts)])

    widened = tokens.astype(jnp.float32)
    normed = (
        widened * lax.rsqrt(jnp.mean(widened * widened, axis=-1, keepdims=True) + norm_eps) * gain
    ).astype(jnp.bfloat16)
    half = BLK // 2
    below = moved(normed, 1)
    above = moved(normed, -1)
    across = jnp.concatenate([moved(above[:half], -1), moved(below[half:], 1)], axis=0)
    places = jnp.array([0, parts - 1, 1, 2], jnp.int32)
    blocks = seq_index * parts + lax.rem(part + places, parts)
    plan, first_position = plan_of(blocks, part, block_owner)
    position = first_position[:, None] + jnp.arange(BLK, dtype=jnp.int32)[None, :]

    def key_values(rows, at):
        count = rows.shape[0]
        keys = rotate(
            jnp.dot(rows, wk, preferred_element_type=jnp.float32).reshape(count, kv_heads, HD), at
        ).astype(jnp.bfloat16)
        values = jnp.dot(rows, wv, preferred_element_type=jnp.float32).astype(jnp.bfloat16)
        own = jnp.concatenate([keys.reshape(count, kv_heads * HD), values], axis=1)
        return with_layout_constraint(own, Layout(major_to_minor=(0, 1)))

    def shared(own):
        return lax.all_gather(own, "seq", axis=0, tiled=True).reshape(-1, BLK, own.shape[1])

    own_part = key_values(normed, position[0])
    beside, own_done = lax.optimization_barrier((jnp.concatenate([below, above], axis=0), own_part))
    beside_part = key_values(beside, position[1:3].reshape(-1))
    across_rows, beside_done = lax.optimization_barrier((across, beside_part))
    across_part = key_values(across_rows, position[3])
    own_kv = shared(own_part)
    beside_part, own_kv = lax.optimization_barrier((beside_part, own_kv))
    beside_kv = shared(beside_part)
    across_part, beside_kv = lax.optimization_barrier((across_part, beside_kv))
    across_kv = shared(across_part)

    def queries_of(rows, at):
        queries = rotate(
            jnp.dot(rows, wq, preferred_element_type=jnp.float32).reshape(BLK, q_heads, HD), at
        )
        queries = (queries * (math.log2(math.e) / math.sqrt(HD))).astype(jnp.bfloat16)
        return queries.reshape(BLK, q_heads * HD)

    pieces = []
    for which, rows, shift in ((3, across, 2), (2, above, 1), (1, below, 3), (0, normed, 0)):
        queries = queries_of(rows, position[which])
        piece = attend(plan[:, which], queries, own_kv, beside_kv, across_kv, wo)
        if shift:
            piece = moved(piece, shift)
        pieces.append(piece)
    total = sum(piece.astype(jnp.float32) for piece in pieces[::-1])
    return total.astype(jnp.bfloat16)


def solution(mesh):
    in_specs = (
        P(("seq", "tensor"), None),
        P(),
        P(None, "tensor"),
        P(None, "tensor"),
        P(None, "tensor"),
        P("tensor", None),
        P(),
    )
    out_specs = P(("seq", "tensor"), None)
    return jax.shard_map(
        per_device, mesh=mesh, in_specs=in_specs, out_specs=out_specs, check_vma=False
    )
```

```python
import functools
import math

import jax
import jax.numpy as jnp
from jax import lax
from jax.experimental import pallas as pl
from jax.experimental.layout import Layout, with_layout_constraint
from jax.experimental.pallas import tpu as pltpu
from jax.sharding import PartitionSpec as P

HD = 128
BLK = 128
LOWEST = -1e30


norm_eps = 1e-05
rope_base = 500000.0


def rotate(vectors, position):
    half_size = vectors.shape[-1] // 2
    exponent = jnp.arange(half_size, dtype=jnp.float32) * (2.0 / vectors.shape[-1])
    frequency = jnp.exp(-exponent * math.log(rope_base))
    angles = position.astype(jnp.float32)[:, None] * frequency[None, :]
    cosine = jnp.cos(angles)[:, None, :]
    sine_part = jnp.sin(angles)[:, None, :]
    first_half = vectors[..., :half_size]
    second = vectors[..., half_size:]
    return jnp.concatenate(
        [first_half * cosine - second * sine_part, second * cosine + first_half * sine_part],
        axis=-1,
    )


def attend_kernel(plan_ref, q_hbm, kv_hbm, wo_hbm, o_ref, qbuf, kvbuf, wobuf, acc, total_s, max_s, kv_sems, q_sem, wo_sem, *, full_blocks, tail_blocks, rows_per_step):
    context, first_own, count, last, part = [plan_ref[i] for i in range(5)]
    heads = qbuf.shape[1] // HD
    groups = kvbuf.shape[3] // (2 * HD)
    per_group = heads // groups
    full_steps = (count - 1) // full_blocks
    rest = count - full_steps * full_blocks
    steps = full_steps + (rest + tail_blocks - 1) // tail_blocks
    wo_copy = pltpu.make_async_copy(wo_hbm, wobuf, wo_sem)
    q_copy = pltpu.make_async_copy(q_hbm, qbuf, q_sem)

    def start_of(step):
        return jnp.where(step < full_steps, step * full_blocks, full_steps * full_blocks + (step - full_steps) * tail_blocks)

    def fetch(step, slot):
        base = start_of(step)

        def one(j):
            at = base + j
            block = jnp.where(at < context, at, jnp.minimum(first_own + at - context, last))
            shard = block // 4
            place = lax.rem(block - part + 4, 4)

            at_shard = jnp.where(place == 3, 1, jnp.where(place == 0, 0, place + 1))
            pltpu.make_async_copy(kv_hbm.at[4 * shard + at_shard], kvbuf.at[slot, j], kv_sems.at[slot]).start()

        def each(j, carry):
            one(j)
            return carry

        lax.fori_loop(0, jnp.where(step < full_steps, full_blocks, tail_blocks), each, 0)

    q_copy.start()
    fetch(0, 0)
    wo_copy.start()
    acc[...] = jnp.zeros_like(acc)
    total_s[...] = jnp.zeros_like(total_s)
    max_s[...] = jnp.full_like(max_s, LOWEST)
    q_copy.wait()

    def absorb(step, blocks, masked):
        slot = lax.rem(step, 2)

        @pl.when(step + 1 < steps)
        def _():
            fetch(step + 1, 1 - slot)

        pltpu.make_async_copy(kv_hbm.at[pl.ds(0, blocks)], kvbuf.at[slot, pl.ds(0, blocks)], kv_sems.at[slot]).wait()
        keys = blocks * BLK
        if masked:
            column = lax.broadcasted_iota(jnp.int32, (BLK, keys), 1) + (start_of(step) - (count - 1)) * BLK
            visible = column <= lax.broadcasted_iota(jnp.int32, (BLK, keys), 0)
            visible = jnp.concatenate([visible] * rows_per_step, axis=0)
        for g in range(groups):
            k = kvbuf[slot, :blocks, :, g * HD:(g + 1) * HD].reshape(keys, HD)
            v = kvbuf[slot, :blocks, :, (groups + g) * HD:(groups + g + 1) * HD].reshape(keys, HD)
            v_one = jnp.concatenate([v, jnp.ones_like(v)], axis=1)
            for first in range(g * per_group, (g + 1) * per_group, rows_per_step):
                q = jnp.concatenate([qbuf[:, h * HD:(h + 1) * HD] for h in range(first, first + rows_per_step)], axis=0)
                s = lax.dot_general(q, k, (((1,), (1,)), ((), ())), preferred_element_type=jnp.float32)
                if masked:
                    s = jnp.where(visible, s, LOWEST)
                rows = pl.ds(first * BLK, rows_per_step * BLK)
                top = s[:, :BLK]
                for j in range(1, blocks):
                    top = jnp.maximum(top, s[:, j * BLK:(j + 1) * BLK])
                old = max_s[rows]
                new = jnp.maximum(old, jnp.max(top, axis=1, keepdims=True))
                factor = jnp.exp2(old - new)
                p = jnp.concatenate([jnp.exp2(s[:, j * BLK:(j + 1) * BLK] - new).astype(jnp.bfloat16) for j in range(blocks)], axis=1)
                r = jnp.dot(p, v_one, preferred_element_type=jnp.float32)
                acc[rows] = acc[rows] * factor + r[:, :HD]
                total_s[rows] = total_s[rows] * factor + r[:, HD:]
                max_s[rows] = new

    def full(step, carry):
        absorb(step, full_blocks, False)
        return carry

    def tail(step, carry):
        absorb(step, tail_blocks, True)
        return carry

    lax.fori_loop(0, full_steps, full, 0)
    lax.fori_loop(full_steps, steps, tail, 0)
    attended = jnp.concatenate(
        [(acc[pl.ds(h * BLK, BLK)] / total_s[pl.ds(h * BLK, BLK)]).astype(jnp.bfloat16) for h in range(heads)], axis=1)
    wo_copy.wait()
    o_ref[...] = jnp.dot(attended, wobuf[...], preferred_element_type=jnp.float32).astype(jnp.bfloat16)


def attend(plan, q, kv, wo, full_blocks=16, tail_blocks=4, rows_per_step=2):
    width = wo.shape[1]
    heads = q.shape[1] // HD
    any_space = pl.BlockSpec(memory_space=pl.ANY)
    state = pltpu.VMEM((heads * BLK, HD), jnp.float32)
    return pl.pallas_call(
        functools.partial(attend_kernel, full_blocks=full_blocks, tail_blocks=tail_blocks, rows_per_step=rows_per_step),
        out_shape=jax.ShapeDtypeStruct((BLK, width), jnp.bfloat16),
        in_specs=[pl.BlockSpec(memory_space=pltpu.SMEM), any_space, any_space, any_space],
        out_specs=pl.BlockSpec(memory_space=pltpu.VMEM),
        scratch_shapes=[
            pltpu.VMEM((BLK, heads * HD), jnp.bfloat16),
            pltpu.VMEM((2, full_blocks, BLK, kv.shape[2]), jnp.bfloat16),
            pltpu.VMEM(wo.shape, jnp.bfloat16),
            state, state, state,
            pltpu.SemaphoreType.DMA((2,)),
            pltpu.SemaphoreType.DMA,
            pltpu.SemaphoreType.DMA,
        ],
        compiler_params=pltpu.CompilerParams(vmem_limit_bytes=56 * 1024 * 1024),
        cost_estimate=pl.CostEstimate(flops=2 * heads * BLK * 6400 * HD, bytes_accessed=4 << 20, transcendentals=0),
    )(plan, q, kv, wo)


def plan_of(blocks, part, owners):
    ids = jnp.arange(owners.shape[0], dtype=jnp.int32)
    owner = jnp.sum(jnp.where(ids[None, :] == blocks[:, None], owners[None, :], 0), axis=1)
    shared = jnp.sum((owners == 0).astype(jnp.int32))
    before = jnp.sum((owners[None, :] < owner[:, None]).astype(jnp.int32), axis=1)
    is_shared = owner == 0
    context = jnp.where(is_shared, blocks + 1, shared)
    count = jnp.where(is_shared, blocks + 1, shared + blocks - before + 1)
    plan = jnp.stack([context, before, count, blocks, jnp.full_like(blocks, part)]).astype(jnp.int32)
    first_position = BLK * jnp.where(is_shared, blocks, shared + blocks - before)
    return plan, first_position


def per_device(tokens, gain, wq, wk, wv, wo, block_owner):
    parts = lax.axis_size("tensor")
    seq_index = lax.axis_index("seq")
    part = lax.axis_index("tensor")
    q_heads = wq.shape[1] // HD
    kv_heads = wk.shape[1] // HD

    def moved(array, shift):
        return lax.ppermute(array, "tensor", [(i, (i + shift) % parts) for i in range(parts)])

    widened = tokens.astype(jnp.float32)
    normed = (
        widened * lax.rsqrt(jnp.mean(widened * widened, axis=-1, keepdims=True) + norm_eps) * gain
    ).astype(jnp.bfloat16)
    half = BLK // 2
    below = moved(normed, 1)
    above = moved(normed, -1)
    across = jnp.concatenate([moved(above[:half], -1), moved(below[half:], 1)], axis=0)
    places = jnp.array([0, parts - 1, 1, 2], jnp.int32)
    blocks = seq_index * parts + lax.rem(part + places, parts)
    plan, first_position = plan_of(blocks, part, block_owner)
    position = first_position[:, None] + jnp.arange(BLK, dtype=jnp.int32)[None, :]

    def key_values(rows, at):
        count = rows.shape[0]
        keys = rotate(
            jnp.dot(rows, wk, preferred_element_type=jnp.float32).reshape(count, kv_heads, HD), at
        ).astype(jnp.bfloat16)
        values = jnp.dot(rows, wv, preferred_element_type=jnp.float32).astype(jnp.bfloat16)
        own = jnp.concatenate([keys.reshape(count, kv_heads * HD), values], axis=1)
        return own

    own = jnp.concatenate(
        [
            key_values(normed, position[0]),
            key_values(jnp.concatenate([below, above], axis=0), position[1:3].reshape(-1)),
            key_values(across, position[3]),
        ],
        axis=0,
    )
    own = with_layout_constraint(own, Layout(major_to_minor=(0, 1)))
    kv = lax.all_gather(own, "seq", axis=0, tiled=True).reshape(-1, BLK, own.shape[1])

    def queries_of(rows, at):
        queries = rotate(
            jnp.dot(rows, wq, preferred_element_type=jnp.float32).reshape(BLK, q_heads, HD), at
        )
        queries = (queries * (math.log2(math.e) / math.sqrt(HD))).astype(jnp.bfloat16)
        return queries.reshape(BLK, q_heads * HD)

    pieces = []
    for which, rows, shift in ((3, across, 2), (2, above, 1), (1, below, 3), (0, normed, 0)):
        queries = queries_of(rows, position[which])
        piece = attend(plan[:, which], queries, kv, wo)
        if shift:
            piece = moved(piece, shift)
        pieces.append(piece)
    total = sum(piece.astype(jnp.float32) for piece in pieces[-1:] + pieces[:-1])
    return total.astype(jnp.bfloat16)


def solution(mesh):
    in_specs = (
        P(("seq", "tensor"), None),
        P(),
        P(None, "tensor"),
        P(None, "tensor"),
        P(None, "tensor"),
        P("tensor", None),
        P(),
    )
    out_specs = P(("seq", "tensor"), None)
    return jax.shard_map(
        per_device, mesh=mesh, in_specs=in_specs, out_specs=out_specs, check_vma=False
    )
```

```python
import functools
import math

import jax
import jax.numpy as jnp
from jax import lax
from jax.experimental import pallas as pl
from jax.experimental.layout import Layout, with_layout_constraint
from jax.experimental.pallas import tpu as pltpu
from jax.sharding import PartitionSpec as P

HD = 128
BLK = 128
LOWEST = -1e30


norm_eps = 1e-05
rope_base = 500000.0


def rotate(vectors, position):
    half_size = vectors.shape[-1] // 2
    exponent = jnp.arange(half_size, dtype=jnp.float32) * (2.0 / vectors.shape[-1])
    frequency = jnp.exp(-exponent * math.log(rope_base))
    angles = position.astype(jnp.float32)[:, None] * frequency[None, :]
    cosine = jnp.cos(angles)[:, None, :]
    sine_part = jnp.sin(angles)[:, None, :]
    first_half = vectors[..., :half_size]
    second = vectors[..., half_size:]
    return jnp.concatenate(
        [first_half * cosine - second * sine_part, second * cosine + first_half * sine_part],
        axis=-1,
    )


def attend_kernel(plan_ref, q_hbm, kv_hbm, wo_hbm, o_ref, qbuf, kvbuf, wobuf, acc, total_s, max_s, kv_sems, q_sem, wo_sem, *, full_blocks, tail_blocks, rows_per_step):
    context, first_own, count, last, part = [plan_ref[i] for i in range(5)]
    heads = qbuf.shape[1] // HD
    groups = kvbuf.shape[3] // (2 * HD)
    per_group = heads // groups
    full_steps = (count - 1) // full_blocks
    rest = count - full_steps * full_blocks
    steps = full_steps + (rest + tail_blocks - 1) // tail_blocks
    wo_copy = pltpu.make_async_copy(wo_hbm, wobuf, wo_sem)
    q_copy = pltpu.make_async_copy(q_hbm, qbuf, q_sem)

    def start_of(step):
        return jnp.where(step < full_steps, step * full_blocks, full_steps * full_blocks + (step - full_steps) * tail_blocks)

    def fetch(step, slot):
        base = start_of(step)

        def one(j):
            at = base + j
            block = jnp.where(at < context, at, jnp.minimum(first_own + at - context, last))
            shard = block // 4
            place = lax.rem(block - part + 4, 4)

            at_shard = jnp.where(place == 3, 1, jnp.where(place == 0, 0, place + 1))
            pltpu.make_async_copy(kv_hbm.at[4 * shard + at_shard], kvbuf.at[slot, j], kv_sems.at[slot]).start()

        def each(j, carry):
            one(j)
            return carry

        lax.fori_loop(0, jnp.where(step < full_steps, full_blocks, tail_blocks), each, 0)

    q_copy.start()
    fetch(0, 0)
    wo_copy.start()
    acc[...] = jnp.zeros_like(acc)
    total_s[...] = jnp.zeros_like(total_s)
    max_s[...] = jnp.full_like(max_s, LOWEST)
    q_copy.wait()

    def absorb(step, blocks, masked):
        slot = lax.rem(step, 2)

        @pl.when(step + 1 < steps)
        def _():
            fetch(step + 1, 1 - slot)

        pltpu.make_async_copy(kv_hbm.at[pl.ds(0, blocks)], kvbuf.at[slot, pl.ds(0, blocks)], kv_sems.at[slot]).wait()
        keys = blocks * BLK
        if masked:
            column = lax.broadcasted_iota(jnp.int32, (BLK, keys), 1) + (start_of(step) - (count - 1)) * BLK
            visible = column <= lax.broadcasted_iota(jnp.int32, (BLK, keys), 0)
            visible = jnp.concatenate([visible] * rows_per_step, axis=0)
        for g in range(groups):
            k = kvbuf[slot, :blocks, :, g * HD:(g + 1) * HD].reshape(keys, HD)
            v = kvbuf[slot, :blocks, :, (groups + g) * HD:(groups + g + 1) * HD].reshape(keys, HD)
            v_one = jnp.concatenate([v, jnp.ones_like(v)], axis=1)
            for first in range(g * per_group, (g + 1) * per_group, rows_per_step):
                q = jnp.concatenate([qbuf[:, h * HD:(h + 1) * HD] for h in range(first, first + rows_per_step)], axis=0)
                s = lax.dot_general(q, k, (((1,), (1,)), ((), ())), preferred_element_type=jnp.float32)
                if masked:
                    s = jnp.where(visible, s, LOWEST)
                rows = pl.ds(first * BLK, rows_per_step * BLK)
                top = s[:, :BLK]
                for j in range(1, blocks):
                    top = jnp.maximum(top, s[:, j * BLK:(j + 1) * BLK])
                old = max_s[rows]
                new = jnp.maximum(old, jnp.max(top, axis=1, keepdims=True))
                factor = jnp.exp2(old - new)
                p = jnp.concatenate([jnp.exp2(s[:, j * BLK:(j + 1) * BLK] - new).astype(jnp.bfloat16) for j in range(blocks)], axis=1)
                r = jnp.dot(p, v_one, preferred_element_type=jnp.float32)
                acc[rows] = acc[rows] * factor + r[:, :HD]
                total_s[rows] = total_s[rows] * factor + r[:, HD:]
                max_s[rows] = new

    def full(step, carry):
        absorb(step, full_blocks, False)
        return carry

    def tail(step, carry):
        absorb(step, tail_blocks, True)
        return carry

    lax.fori_loop(0, full_steps, full, 0)
    lax.fori_loop(full_steps, steps, tail, 0)
    attended = jnp.concatenate(
        [(acc[pl.ds(h * BLK, BLK)] / total_s[pl.ds(h * BLK, BLK)]).astype(jnp.bfloat16) for h in range(heads)], axis=1)
    wo_copy.wait()
    o_ref[...] = jnp.dot(attended, wobuf[...], preferred_element_type=jnp.float32).astype(jnp.bfloat16)


def attend(plan, q, kv, wo, full_blocks=16, tail_blocks=4, rows_per_step=1):
    width = wo.shape[1]
    heads = q.shape[1] // HD
    any_space = pl.BlockSpec(memory_space=pl.ANY)
    state = pltpu.VMEM((heads * BLK, HD), jnp.float32)
    return pl.pallas_call(
        functools.partial(attend_kernel, full_blocks=full_blocks, tail_blocks=tail_blocks, rows_per_step=rows_per_step),
        out_shape=jax.ShapeDtypeStruct((BLK, width), jnp.bfloat16),
        in_specs=[pl.BlockSpec(memory_space=pltpu.SMEM), any_space, any_space, any_space],
        out_specs=pl.BlockSpec(memory_space=pltpu.VMEM),
        scratch_shapes=[
            pltpu.VMEM((BLK, heads * HD), jnp.bfloat16),
            pltpu.VMEM((2, full_blocks, BLK, kv.shape[2]), jnp.bfloat16),
            pltpu.VMEM(wo.shape, jnp.bfloat16),
            state, state, state,
            pltpu.SemaphoreType.DMA((2,)),
            pltpu.SemaphoreType.DMA,
            pltpu.SemaphoreType.DMA,
        ],
        compiler_params=pltpu.CompilerParams(vmem_limit_bytes=56 * 1024 * 1024),
        cost_estimate=pl.CostEstimate(flops=2 * heads * BLK * 6400 * HD, bytes_accessed=4 << 20, transcendentals=0),
    )(plan, q, kv, wo)


def plan_of(blocks, part, owners):
    ids = jnp.arange(owners.shape[0], dtype=jnp.int32)
    owner = jnp.sum(jnp.where(ids[None, :] == blocks[:, None], owners[None, :], 0), axis=1)
    shared = jnp.sum((owners == 0).astype(jnp.int32))
    before = jnp.sum((owners[None, :] < owner[:, None]).astype(jnp.int32), axis=1)
    is_shared = owner == 0
    context = jnp.where(is_shared, blocks + 1, shared)
    count = jnp.where(is_shared, blocks + 1, shared + blocks - before + 1)
    plan = jnp.stack([context, before, count, blocks, jnp.full_like(blocks, part)]).astype(jnp.int32)
    first_position = BLK * jnp.where(is_shared, blocks, shared + blocks - before)
    return plan, first_position


def per_device(tokens, gain, wq, wk, wv, wo, block_owner):
    parts = lax.axis_size("tensor")
    seq_index = lax.axis_index("seq")
    part = lax.axis_index("tensor")
    q_heads = wq.shape[1] // HD
    kv_heads = wk.shape[1] // HD

    def moved(array, shift):
        return lax.ppermute(array, "tensor", [(i, (i + shift) % parts) for i in range(parts)])

    widened = tokens.astype(jnp.float32)
    normed = (
        widened * lax.rsqrt(jnp.mean(widened * widened, axis=-1, keepdims=True) + norm_eps) * gain
    ).astype(jnp.bfloat16)
    half = BLK // 2
    below = moved(normed, 1)
    above = moved(normed, -1)
    across = jnp.concatenate([moved(above[:half], -1), moved(below[half:], 1)], axis=0)
    places = jnp.array([0, parts - 1, 1, 2], jnp.int32)
    blocks = seq_index * parts + lax.rem(part + places, parts)
    plan, first_position = plan_of(blocks, part, block_owner)
    position = first_position[:, None] + jnp.arange(BLK, dtype=jnp.int32)[None, :]

    def key_values(rows, at):
        count = rows.shape[0]
        keys = rotate(
            jnp.dot(rows, wk, preferred_element_type=jnp.float32).reshape(count, kv_heads, HD), at
        ).astype(jnp.bfloat16)
        values = jnp.dot(rows, wv, preferred_element_type=jnp.float32).astype(jnp.bfloat16)
        own = jnp.concatenate([keys.reshape(count, kv_heads * HD), values], axis=1)
        return own

    own = jnp.concatenate(
        [
            key_values(normed, position[0]),
            key_values(jnp.concatenate([below, above], axis=0), position[1:3].reshape(-1)),
            key_values(across, position[3]),
        ],
        axis=0,
    )
    own = with_layout_constraint(own, Layout(major_to_minor=(0, 1)))
    kv = lax.all_gather(own, "seq", axis=0, tiled=True).reshape(-1, BLK, own.shape[1])

    def queries_of(rows, at):
        queries = rotate(
            jnp.dot(rows, wq, preferred_element_type=jnp.float32).reshape(BLK, q_heads, HD), at
        )
        queries = (queries * (math.log2(math.e) / math.sqrt(HD))).astype(jnp.bfloat16)
        return queries.reshape(BLK, q_heads * HD)

    pieces = []
    for which, rows, shift in ((3, across, 2), (2, above, 1), (1, below, 3), (0, normed, 0)):
        queries = queries_of(rows, position[which])
        piece = attend(plan[:, which], queries, kv, wo)
        if shift:
            piece = moved(piece, shift)
        pieces.append(piece)
    total = sum(piece.astype(jnp.float32) for piece in pieces[-1:] + pieces[:-1])
    return total.astype(jnp.bfloat16)


def solution(mesh):
    in_specs = (
        P(("seq", "tensor"), None),
        P(),
        P(None, "tensor"),
        P(None, "tensor"),
        P(None, "tensor"),
        P("tensor", None),
        P(),
    )
    out_specs = P(("seq", "tensor"), None)
    return jax.shard_map(
        per_device, mesh=mesh, in_specs=in_specs, out_specs=out_specs, check_vma=False
    )
```
